16 devices in a mesh: data: 2 (over z), tensor: 8 (over y, x, core).
Axes of the slice: x: 2, y: 2, z: 2, core: 2. Of those that a mesh axis runs over, the one named last changes fastest.
Arguments:
- x_in: bfloat16 [64, 128, 5120], P('data'), parts along dimension 0
- adapter_ids: int32 [64], P('data'), parts along dimension 0
- gain_attn: float32 [5120], replicated
- gain_mlp: float32 [5120], replicated
- w_q: bfloat16 [5120, 40, 128], P(None, 'tensor')
- w_k: bfloat16 [5120, 40, 128], P(None, 'tensor')
- w_v: bfloat16 [5120, 40, 128], P(None, 'tensor')
- w_o: bfloat16 [40, 128, 5120], P('tensor')
- w_gate: bfloat16 [5120, 13824], P(None, 'tensor')
- w_up: bfloat16 [5120, 13824], P(None, 'tensor')
- w_down: bfloat16 [13824, 5120], P('tensor')
- a_q: bfloat16 [8, 5120, 256], P(None, None, 'tensor')
- b_q: bfloat16 [8, 256, 40, 128], P(None, None, 'tensor')
- a_k: bfloat16 [8, 5120, 256], P(None, None, 'tensor')
- b_k: bfloat16 [8, 256, 40, 128], P(None, None, 'tensor')
- a_v: bfloat16 [8, 5120, 256], P(None, None, 'tensor')
- b_v: bfloat16 [8, 256, 40, 128], P(None, None, 'tensor')
- a_o: bfloat16 [8, 40, 128, 256], P(None, 'tensor')
- b_o: bfloat16 [8, 256, 5120], P(None, None, 'tensor')
- a_gate: bfloat16 [8, 5120, 256], P(None, None, 'tensor')
- b_gate: bfloat16 [8, 256, 13824], P(None, None, 'tensor')
- a_up: bfloat16 [8, 5120, 256], P(None, None, 'tensor')
- b_up: bfloat16 [8, 256, 13824], P(None, None, 'tensor')
- a_down: bfloat16 [8, 13824, 256], P(None, 'tensor')
- b_down: bfloat16 [8, 256, 5120], P(None, None, 'tensor')
Outputs:
- output: bfloat16 [64, 128, 5120], P('data'), parts along dimension 0
There are 2 independent parts. The reference program is written for one: setup_inputs(seed, part) draws one part's arguments, and reference() takes and returns one part's arrays. A program takes and returns all parts, laid end to end along the dimension named above; an argument that names none is the same for every part.
All inputs are finite; a program needn't handle non-finite values.
Results may differ from the reference program's by a relative error of at most 0.02.
Values are sent between devices in bfloat16 or wider.
A program may use at most 1 GiB of HBM per device.

```python
import jax
import jax.numpy as jnp
from jax import lax

MODEL_DIM = 5120
FFN_DIM = 13824
NUM_HEADS = 40
KV_HEADS = 40
HEAD_DIM = 128
BATCH = 32
SEQ_LEN = 128
RANK = 256
ADAPTERS = 8
ALPHA = 16
ROPE_BASE = 10000

Q_WIDTH = NUM_HEADS * HEAD_DIM
KV_WIDTH = KV_HEADS * HEAD_DIM
GROUP_SIZE = NUM_HEADS // KV_HEADS
LORA_SCALE = ALPHA / RANK
EPSILON = 1e-5


def draw_ids(key_in):
    key_first, key_second, key_perm = jax.random.split(key_in, 3)
    first_draw = jax.random.randint(key_first, (BATCH,), 0, ADAPTERS)
    second_draw = jax.random.randint(key_second, (BATCH,), 0, ADAPTERS)
    slot_index = jnp.arange(BATCH)
    chosen = jnp.where(slot_index < ADAPTERS, slot_index, jnp.minimum(first_draw, second_draw))
    return jax.random.permutation(key_perm, chosen).astype(jnp.int32)


def setup_inputs(seed: int = 0, part: int = 0) -> dict:
    root_key = jax.random.key(seed)
    key_x, key_ids = jax.random.split(jax.random.fold_in(root_key, part), 2)
    key_list = jax.random.split(root_key, 23)
    b_scale = 0.2 * RANK ** 0.5 / ALPHA

    def normal_bf16(key_in, arr_shape, scale_val):
        return (jax.random.normal(key_in, arr_shape, jnp.float32) * scale_val).astype(jnp.bfloat16)

    return {
        'x_in': normal_bf16(key_x, (BATCH, SEQ_LEN, MODEL_DIM), 1.0),
        'adapter_ids': draw_ids(key_ids),
        'gain_attn': 1.0 + 0.25 * jax.random.normal(key_list[0], (MODEL_DIM,), jnp.float32),
        'gain_mlp': 1.0 + 0.25 * jax.random.normal(key_list[1], (MODEL_DIM,), jnp.float32),
        'w_q': normal_bf16(key_list[2], (MODEL_DIM, NUM_HEADS, HEAD_DIM), 1.6 * MODEL_DIM ** -0.5),
        'w_k': normal_bf16(key_list[3], (MODEL_DIM, KV_HEADS, HEAD_DIM), 1.6 * MODEL_DIM ** -0.5),
        'w_v': normal_bf16(key_list[4], (MODEL_DIM, KV_HEADS, HEAD_DIM), MODEL_DIM ** -0.5),
        'w_o': normal_bf16(key_list[5], (NUM_HEADS, HEAD_DIM, MODEL_DIM), 1.4 * Q_WIDTH ** -0.5),
        'w_gate': normal_bf16(key_list[6], (MODEL_DIM, FFN_DIM), MODEL_DIM ** -0.5),
        'w_up': normal_bf16(key_list[7], (MODEL_DIM, FFN_DIM), MODEL_DIM ** -0.5),
        'w_down': normal_bf16(key_list[8], (FFN_DIM, MODEL_DIM), 1.4 * FFN_DIM ** -0.5),
        'a_q': normal_bf16(key_list[9], (ADAPTERS, MODEL_DIM, RANK), MODEL_DIM ** -0.5),
        'b_q': normal_bf16(key_list[10], (ADAPTERS, RANK, NUM_HEADS, HEAD_DIM), 1.6 * b_scale),
        'a_k': normal_bf16(key_list[11], (ADAPTERS, MODEL_DIM, RANK), MODEL_DIM ** -0.5),
        'b_k': normal_bf16(key_list[12], (ADAPTERS, RANK, KV_HEADS, HEAD_DIM), 1.6 * b_scale),
        'a_v': normal_bf16(key_list[13], (ADAPTERS, MODEL_DIM, RANK), MODEL_DIM ** -0.5),
        'b_v': normal_bf16(key_list[14], (ADAPTERS, RANK, KV_HEADS, HEAD_DIM), b_scale),
        'a_o': normal_bf16(key_list[15], (ADAPTERS, NUM_HEADS, HEAD_DIM, RANK), Q_WIDTH ** -0.5),
        'b_o': normal_bf16(key_list[16], (ADAPTERS, RANK, MODEL_DIM), 1.4 * b_scale),
        'a_gate': normal_bf16(key_list[17], (ADAPTERS, MODEL_DIM, RANK), MODEL_DIM ** -0.5),
        'b_gate': normal_bf16(key_list[18], (ADAPTERS, RANK, FFN_DIM), b_scale),
        'a_up': normal_bf16(key_list[19], (ADAPTERS, MODEL_DIM, RANK), MODEL_DIM ** -0.5),
        'b_up': normal_bf16(key_list[20], (ADAPTERS, RANK, FFN_DIM), b_scale),
        'a_down': normal_bf16(key_list[21], (ADAPTERS, FFN_DIM, RANK), FFN_DIM ** -0.5),
        'b_down': normal_bf16(key_list[22], (ADAPTERS, RANK, MODEL_DIM), 1.4 * b_scale),
    }


def rms_gain(act_in, gain_vec):
    act_f32 = act_in.astype(jnp.float32)
    inv_rms = lax.rsqrt(jnp.mean(act_f32 * act_f32, axis=-1, keepdims=True) + EPSILON)
    return (act_f32 * inv_rms * gain_vec).astype(jnp.bfloat16)


def rope_rotate(head_vals):
    half_dim = HEAD_DIM // 2
    inv_freq = ROPE_BASE ** (-2.0 * jnp.arange(half_dim, dtype=jnp.float32) / HEAD_DIM)
    angle_tab = jnp.arange(SEQ_LEN, dtype=jnp.float32)[:, None] * inv_freq[None, :]
    cos_tab = jnp.cos(angle_tab)[:, None, :]
    sin_tab = jnp.sin(angle_tab)[:, None, :]
    first_half = head_vals[..., :half_dim]
    second_half = head_vals[..., half_dim:]
    return jnp.concatenate([first_half * cos_tab - second_half * sin_tab, second_half * cos_tab + first_half * sin_tab], axis=-1)


def reference(x_in, adapter_ids, gain_attn, gain_mlp, w_q, w_k, w_v, w_o, w_gate, w_up, w_down, a_q, b_q, a_k, b_k, a_v, b_v, a_o, b_o, a_gate, b_gate, a_up, b_up, a_down, b_down):
    flat_q = w_q.reshape(MODEL_DIM, Q_WIDTH)
    flat_k = w_k.reshape(MODEL_DIM, KV_WIDTH)
    flat_v = w_v.reshape(MODEL_DIM, KV_WIDTH)
    flat_o = w_o.reshape(Q_WIDTH, MODEL_DIM)
    causal = jnp.arange(SEQ_LEN)[:, None] >= jnp.arange(SEQ_LEN)[None, :]

    def project(act_in, weight, a_mat, b_mat):
        base_out = jnp.dot(act_in, weight, preferred_element_type=jnp.float32)
        low_rank = jnp.dot(act_in, a_mat, preferred_element_type=jnp.float32).astype(jnp.bfloat16)
        return base_out + LORA_SCALE * jnp.dot(low_rank, b_mat, preferred_element_type=jnp.float32)

    def one_sequence(seq_pair):
        x_seq, adapter = seq_pair
        h_attn = rms_gain(x_seq, gain_attn)
        z_q = project(h_attn, flat_q, a_q[adapter], b_q[adapter].reshape(RANK, Q_WIDTH))
        z_k = project(h_attn, flat_k, a_k[adapter], b_k[adapter].reshape(RANK, KV_WIDTH))
        z_v = project(h_attn, flat_v, a_v[adapter], b_v[adapter].reshape(RANK, KV_WIDTH))
        q_heads = rope_rotate(z_q.reshape(SEQ_LEN, NUM_HEADS, HEAD_DIM)).astype(jnp.bfloat16)
        k_heads = rope_rotate(z_k.reshape(SEQ_LEN, KV_HEADS, HEAD_DIM)).astype(jnp.bfloat16)
        v_heads = z_v.reshape(SEQ_LEN, KV_HEADS, HEAD_DIM).astype(jnp.bfloat16)
        q_group = q_heads.reshape(SEQ_LEN, KV_HEADS, GROUP_SIZE, HEAD_DIM)
        scores = jnp.einsum('skgd,tkd->kgst', q_group.astype(jnp.float32), k_heads.astype(jnp.float32)) * HEAD_DIM ** -0.5
        attn_prob = jax.nn.softmax(jnp.where(causal, scores, -1e30), axis=-1).astype(jnp.bfloat16)
        mixed_out = jnp.einsum('kgst,tkd->skgd', attn_prob.astype(jnp.float32), v_heads.astype(jnp.float32))
        attn_out = mixed_out.astype(jnp.bfloat16).reshape(SEQ_LEN, Q_WIDTH)
        z_o = project(attn_out, flat_o, a_o[adapter].reshape(Q_WIDTH, RANK), b_o[adapter])
        x_mid = (x_seq.astype(jnp.float32) + z_o).astype(jnp.bfloat16)
        h_mlp = rms_gain(x_mid, gain_mlp)
        z_gate = project(h_mlp, w_gate, a_gate[adapter], b_gate[adapter])
        z_up = project(h_mlp, w_up, a_up[adapter], b_up[adapter])
        hidden = (jax.nn.silu(z_gate) * z_up).astype(jnp.bfloat16)
        z_down = project(hidden, w_down, a_down[adapter], b_down[adapter])
        return (x_mid.astype(jnp.float32) + z_down).astype(jnp.bfloat16)

    return lax.map(one_sequence, (x_in, adapter_ids))
```

```python
import jax
import jax.numpy as jnp
from jax import lax
from jax.experimental import pallas as pl
from jax.experimental.pallas import tpu as pltpu
from jax.sharding import PartitionSpec as P

ALPHA = 16.0
ROPE_BASE = 10000.0
EPSILON = 1e-5
CHUNKS = 4


def rms_gain(act_in, gain_vec):
    act_f32 = act_in.astype(jnp.float32)
    inv_rms = lax.rsqrt(jnp.mean(act_f32 * act_f32, axis=-1, keepdims=True) + EPSILON)
    return (act_f32 * inv_rms * gain_vec).astype(jnp.bfloat16)


def rope_rotate(head_vals):
    seq_len = head_vals.shape[1]
    head_dim = head_vals.shape[-1]
    half_dim = head_dim // 2
    inv_freq = ROPE_BASE ** (-2.0 * jnp.arange(half_dim, dtype=jnp.float32) / head_dim)
    angle_tab = jnp.arange(seq_len, dtype=jnp.float32)[:, None] * inv_freq[None, :]
    cos_tab = jnp.cos(angle_tab)[:, None, :]
    sin_tab = jnp.sin(angle_tab)[:, None, :]
    first_half = head_vals[..., :half_dim]
    second_half = head_vals[..., half_dim:]
    return jnp.concatenate([first_half * cos_tab - second_half * sin_tab, second_half * cos_tab + first_half * sin_tab], axis=-1)


def causal_attention(q_heads, k_heads, v_heads):
    head_dim = q_heads.shape[-1]
    seq_len = q_heads.shape[1]
    scores = jnp.einsum('bshd,bthd->bhst', q_heads, k_heads, preferred_element_type=jnp.float32) * head_dim ** -0.5
    causal = jnp.arange(seq_len)[:, None] >= jnp.arange(seq_len)[None, :]
    attn_prob = jax.nn.softmax(jnp.where(causal, scores, -1e30), axis=-1).astype(jnp.bfloat16)
    mixed_out = jnp.einsum('bhst,bthd->bshd', attn_prob, v_heads, preferred_element_type=jnp.float32)
    return mixed_out.astype(jnp.bfloat16)


COLS = 256
ROWS = 512


def gate_up_kernel(ids_ref, h_ref, low_gate_ref, low_up_ref, w_gate_ref, w_up_ref, b_gate_ref, b_up_ref, out_ref):
    seq_len = 128
    for first in range(0, h_ref.shape[0], ROWS):
        rows = pl.ds(first, ROWS)

        def proj(w_ref, b_ref, low_ref):
            deltas = []
            for start in range(first, first + ROWS, seq_len):
                adapter = ids_ref[start // seq_len]
                deltas.append(jnp.dot(low_ref[pl.ds(start, seq_len), :], b_ref[adapter], preferred_element_type=jnp.float32))
            base = jnp.dot(h_ref[rows, :], w_ref[...], preferred_element_type=jnp.float32)
            return base + jnp.concatenate(deltas, axis=0)

        z_gate = proj(w_gate_ref, b_gate_ref, low_gate_ref)
        z_up = proj(w_up_ref, b_up_ref, low_up_ref)
        out_ref[rows, :] = (z_gate * jax.nn.sigmoid(z_gate) * z_up).astype(out_ref.dtype)


def gate_up(ids, h, low_gate, low_up, w_gate, w_up, b_gate, b_up):
    rows, width = h.shape
    cols = w_gate.shape[1]
    adapters, rank = b_gate.shape[:2]
    whole = lambda shape: pl.BlockSpec(shape, lambda n, ids: (0,) * len(shape), pipeline_mode=pl.Buffered(1))
    w_spec = pl.BlockSpec((width, COLS), lambda n, ids: (0, n))
    b_spec = pl.BlockSpec((adapters, rank, COLS), lambda n, ids: (0, 0, n))
    flops = 4 * rows * (width + rank) * cols
    return pl.pallas_call(
        gate_up_kernel,
        out_shape=jax.ShapeDtypeStruct((rows, cols), jnp.bfloat16),
        grid_spec=pltpu.PrefetchScalarGridSpec(
            num_scalar_prefetch=1,
            grid=(pl.cdiv(cols, COLS),),
            in_specs=[whole((rows, width)), whole((rows, rank)), whole((rows, rank)), w_spec, w_spec, b_spec, b_spec],
            out_specs=pl.BlockSpec((rows, COLS), lambda n, ids: (0, n)),
        ),
        compiler_params=pltpu.CompilerParams(dimension_semantics=('arbitrary',), vmem_limit_bytes=44 * 1024 * 1024),
        cost_estimate=pl.CostEstimate(flops=flops, bytes_accessed=4 * width * cols + 2 * rows * (width + cols), transcendentals=rows * cols),
    )(ids, h, low_gate, low_up, w_gate, w_up, b_gate, b_up)


def solution(mesh):
    tp_size = mesh.shape['tensor']
    head_split = P(None, 'tensor', None)
    last_split = P(None, None, 'tensor')
    b_head_split = P(None, None, 'tensor', None)
    in_specs = (P('data', None, None), P('data'), P(None), P(None),
                head_split, head_split, head_split, P('tensor', None, None),
                P(None, 'tensor'), P(None, 'tensor'), P('tensor', None),
                last_split, b_head_split, last_split, b_head_split, last_split, b_head_split,
                P(None, 'tensor', None, None), last_split,
                last_split, last_split, last_split, last_split,
                P(None, 'tensor', None), last_split)

    def local_layer(x_in, adapter_ids, gain_attn, gain_mlp, w_q, w_k, w_v, w_o, w_gate, w_up, w_down, a_q, b_q, a_k, b_k, a_v, b_v, a_o, b_o, a_gate, b_gate, a_up, b_up, a_down, b_down):
        batch, seq_len, width = x_in.shape
        adapters, rank = b_q.shape[:2]
        rank_part = rank // tp_size
        scale = ALPHA / rank
        per_chunk = batch // CHUNKS
        my_index = lax.axis_index('tensor')
        shard_width = width // tp_size
        flat_b = lambda b: b.reshape((adapters * rank,) + b.shape[2:])

        def stack_a(*stacks):
            return jnp.concatenate([a.transpose(1, 0, 2).reshape(width, adapters * rank_part) for a in stacks], axis=1)

        a_qkv = stack_a(a_q, a_k, a_v)
        a_gu = stack_a(a_gate, a_up)

        def expand(low, hot):
            low = low * jnp.asarray(scale, jnp.bfloat16)
            wide = jnp.where(hot[:, None, :, None], low[:, :, None, :], jnp.zeros((), jnp.bfloat16))
            return wide.reshape(per_chunk, seq_len, adapters * rank)

        own = per_chunk // tp_size
        last = [adapter_ids]

        def gate(value):
            return lax.optimization_barrier((value, last[0]))[0]

        def mark(value):
            last[0] = value
            return value

        def low_own(act, a_all, count, hot):
            low = jnp.einsum('bsd,dn->bsn', act, a_all, preferred_element_type=jnp.float32)
            low = low.reshape(per_chunk, seq_len, count, adapters, rank_part)
            low = jnp.sum(jnp.where(hot[:, None, None, :, None], low, 0.0), axis=3).astype(jnp.bfloat16)
            return low.reshape(per_chunk, seq_len, count * rank_part)

        def low_all(low, count):
            full = lax.all_gather(low, 'tensor', axis=0)
            full = full.reshape(tp_size, per_chunk, seq_len, count, rank_part)
            return full.transpose(3, 1, 2, 0, 4).reshape(count, per_chunk, seq_len, rank)

        def swap(value, bit):
            return lax.ppermute(value, 'tensor', [(i, i ^ bit) for i in range(tp_size)])

        def pick(value, index, axis):
            return lax.squeeze(lax.dynamic_slice_in_dim(value, index, 1, axis=axis), (axis,))

        def add(left, right):
            return (left.astype(jnp.float32) + right.astype(jnp.float32)).astype(jnp.bfloat16)

        core, col, row = my_index % 2, (my_index // 2) % 2, my_index // 4

        def low_sum(low_part):
            for bit in (1, 2, 4):
                low_part = add(low_part, swap(low_part, bit))
            return low_part

        def scatter_sum(part):
            half = seq_len // 2
            part = part.reshape(4, 2, seq_len, width)
            got = swap(pick(part, 1 - core, 1), 1)
            part = add(pick(part, core, 1), got).reshape(2, 2, seq_len, width)
            by_col, by_row = part[:, :, :half], part[:, :, half:]
            got_col = swap(pick(by_col, 1 - col, 1), 2)
            got_row = swap(pick(by_row, 1 - row, 0), 4)
            by_col = add(pick(by_col, col, 1), got_col)
            by_row = add(pick(by_row, row, 0), got_row)
            got_col = swap(pick(by_col, 1 - row, 0), 4)
            got_row = swap(pick(by_row, 1 - col, 0), 2)
            by_col = add(pick(by_col, row, 0), got_col)
            by_row = add(pick(by_row, col, 0), got_row)
            return jnp.concatenate([by_col, by_row], axis=0)[None]

        def chunk_of(c):
            ids = lax.slice_in_dim(adapter_ids, c * per_chunk, (c + 1) * per_chunk)
            return ids, ids[:, None] == jnp.arange(adapters)[None, :]

        def attn_low(c):
            x_c = lax.slice_in_dim(gate(x_in), c * per_chunk, (c + 1) * per_chunk)
            h_attn = rms_gain(x_c, gain_attn)
            low = mark(low_own(h_attn, a_qkv, 3, chunk_of(c)[1]))
            return h_attn, low_all(low, 3)

        def attn_mix(c, h_attn, low_qkv):
            ids, hot = chunk_of(c)
            h_attn = gate(h_attn)

            def proj(weight, b_stack, low):
                base = jnp.einsum('bsd,dhe->bshe', h_attn, weight, preferred_element_type=jnp.float32)
                return base + jnp.einsum('bsk,khe->bshe', expand(low, hot), flat_b(b_stack), preferred_element_type=jnp.float32)

            q = rope_rotate(proj(w_q, b_q, low_qkv[0])).astype(jnp.bfloat16)
            k = rope_rotate(proj(w_k, b_k, low_qkv[1])).astype(jnp.bfloat16)
            v = proj(w_v, b_v, low_qkv[2]).astype(jnp.bfloat16)
            attn_out = causal_attention(q, k, v)
            a_sel = jnp.take(a_o, ids, axis=0, mode='clip')
            low_part = jnp.einsum('bshe,bher->bsr', attn_out, a_sel, preferred_element_type=jnp.float32).astype(jnp.bfloat16)
            return attn_out, low_sum(mark(low_part))

        def row_part(c, act, weight, low, b_stack, base_form):
            base = jnp.einsum(base_form, gate(act), weight, preferred_element_type=jnp.float32).astype(jnp.bfloat16)
            delta = jnp.einsum('bsk,kd->bsd', expand(low, chunk_of(c)[1]), flat_b(b_stack), preferred_element_type=jnp.float32)
            start = my_index * shard_width
            mine = lax.dynamic_slice_in_dim(base, start, shard_width, axis=2)
            mine = (mine.astype(jnp.float32) + delta).astype(jnp.bfloat16)
            part = mark(lax.dynamic_update_slice_in_dim(base, mine, start, axis=2))
            return scatter_sum(part)

        def mid_own(c, z_o):
            x_own = lax.dynamic_slice_in_dim(x_in, c * per_chunk + my_index * own, own, axis=0)
            x_mid = (x_own.astype(jnp.float32) + gate(z_o).astype(jnp.float32)).astype(jnp.bfloat16)
            h_own = mark(rms_gain(x_mid, gain_mlp))
            return x_mid, lax.all_gather(h_own, 'tensor', axis=0, tiled=True)

        def mlp_low(c, h_mlp):
            low = mark(low_own(gate(h_mlp), a_gu, 2, chunk_of(c)[1]))
            return low_all(low, 2)

        def mlp_mix(c, h_mlp, low_gu):
            ids, hot = chunk_of(c)
            h_mlp = gate(h_mlp)

            flat = lambda v: v.reshape(per_chunk * seq_len, v.shape[-1])
            low_gu = low_gu * jnp.asarray(scale, jnp.bfloat16)
            hidden = gate_up(ids, flat(h_mlp), flat(low_gu[0]), flat(low_gu[1]), w_gate, w_up, b_gate, b_up)
            hidden = hidden.reshape(per_chunk, seq_len, hidden.shape[-1])
            a_sel = jnp.take(a_down, ids, axis=0, mode='clip')
            low_part = jnp.einsum('bsf,bfr->bsr', hidden, a_sel, preferred_element_type=jnp.float32).astype(jnp.bfloat16)
            return hidden, low_sum(mark(low_part))

        def out_own(c, z_down):
            y_own = mark((mid[c].astype(jnp.float32) + gate(z_down).astype(jnp.float32)).astype(jnp.bfloat16))
            return lax.all_gather(y_own, 'tensor', axis=0, tiled=True)

        pre, mid, h_mlp, z_o, pre_gu, z_down, y_all = {}, {}, {}, {}, {}, {}, {}
        act, low_sums = {}, {}
        pre[0] = attn_low(0)
        for c in range(CHUNKS + 1):
            if c + 1 < CHUNKS:
                pre[c + 1] = attn_low(c + 1)
            if c < CHUNKS:
                act[c], low_sums[c] = attn_mix(c, *pre[c])
            if c >= 1:
                z_o[c - 1] = row_part(c - 1, act[c - 1], w_o, low_sums[c - 1], b_o, 'bshe,hed->bsd')
            if c >= 2:
                mid[c - 2], h_mlp[c - 2] = mid_own(c - 2, z_o[c - 2])
        for c in range(CHUNKS + 1):
            if c < CHUNKS:
                pre_gu[c] = mlp_low(c, h_mlp[c])
            if c >= 1:
                z_down[c - 1] = row_part(c - 1, act[c - 1], w_down, low_sums[c - 1], b_down, 'bsf,fd->bsd')
            if c == 0:
                mid[CHUNKS - 1], h_mlp[CHUNKS - 1] = mid_own(CHUNKS - 1, z_o[CHUNKS - 1])
            if c < CHUNKS:
                act[c], low_sums[c] = mlp_mix(c, h_mlp[c], pre_gu[c])
            if c >= 2:
                y_all[c - 2] = out_own(c - 2, z_down[c - 2])
        y_all[CHUNKS - 1] = out_own(CHUNKS - 1, z_down[CHUNKS - 1])
        return jnp.concatenate([y_all[c] for c in range(CHUNKS)], axis=0)

    return jax.shard_map(local_layer, mesh=mesh, in_specs=in_specs, out_specs=P('data', None, None), check_vma=False)
```

```python
import jax
import jax.numpy as jnp
from jax import lax
from jax.experimental import pallas as pl
from jax.experimental.pallas import tpu as pltpu
from jax.sharding import PartitionSpec as P

ALPHA = 16.0
ROPE_BASE = 10000.0
EPSILON = 1e-5
CHUNKS = 4


def rms_gain(act_in, gain_vec):
    act_f32 = act_in.astype(jnp.float32)
    inv_rms = lax.rsqrt(jnp.mean(act_f32 * act_f32, axis=-1, keepdims=True) + EPSILON)
    return (act_f32 * inv_rms * gain_vec).astype(jnp.bfloat16)


def rope_tables(seq_len, head_dim):
    half_dim = head_dim // 2
    inv_freq = ROPE_BASE ** (-2.0 * jnp.arange(half_dim, dtype=jnp.float32) / head_dim)
    angle_tab = jnp.arange(seq_len, dtype=jnp.float32)[:, None] * inv_freq[None, :]
    cos_tab, sin_tab = jnp.cos(angle_tab), jnp.sin(angle_tab)
    return jnp.concatenate([cos_tab, cos_tab], axis=-1), jnp.concatenate([-sin_tab, sin_tab], axis=-1)


COLS = 256
NT = (((1,), (1,)), ((), ()))
VMEM_LIMIT = 46 * 1024 * 1024


def whole(shape):
    return pl.BlockSpec(shape, lambda n, ids: (0,) * len(shape), pipeline_mode=pl.Buffered(1))


def gate_up_kernel(ids_ref, h_ref, low_gate_ref, low_up_ref, w_gate_ref, w_up_ref, b_gate_ref, b_up_ref, out_ref):
    rows = h_ref.shape[0]
    seq_len = rows // ids_ref.shape[0]

    def proj(w_ref, b_ref, low_ref):
        deltas = []
        for seq in range(rows // seq_len):
            low = low_ref[pl.ds(seq * seq_len, seq_len), :]
            deltas.append(lax.dot_general(low, b_ref[ids_ref[seq]], NT, preferred_element_type=jnp.float32))
        base = lax.dot_general(h_ref[...], w_ref[...], NT, preferred_element_type=jnp.float32)
        return base + jnp.concatenate(deltas, axis=0)

    z_gate = proj(w_gate_ref, b_gate_ref, low_gate_ref)
    z_up = proj(w_up_ref, b_up_ref, low_up_ref)
    out_ref[...] = (z_gate * jax.nn.sigmoid(z_gate) * z_up).astype(out_ref.dtype)


def gate_up(ids, h, low_gate, low_up, w_gate, w_up, b_gate, b_up):
    rows, width = h.shape
    cols = w_gate.shape[0]
    adapters, _, rank = b_gate.shape
    w_spec = pl.BlockSpec((COLS, width), lambda n, ids: (n, 0))
    b_spec = pl.BlockSpec((adapters, COLS, rank), lambda n, ids: (0, n, 0))
    flops = 4 * rows * (width + rank) * cols
    return pl.pallas_call(
        gate_up_kernel,
        out_shape=jax.ShapeDtypeStruct((rows, cols), jnp.bfloat16),
        grid_spec=pltpu.PrefetchScalarGridSpec(
            num_scalar_prefetch=1,
            grid=(pl.cdiv(cols, COLS),),
            in_specs=[whole((rows, width)), whole((rows, rank)), whole((rows, rank)), w_spec, w_spec, b_spec, b_spec],
            out_specs=pl.BlockSpec((rows, COLS), lambda n, ids: (0, n)),
        ),
        compiler_params=pltpu.CompilerParams(dimension_semantics=('arbitrary',), vmem_limit_bytes=VMEM_LIMIT),
        cost_estimate=pl.CostEstimate(flops=flops, bytes_accessed=4 * width * cols + 2 * rows * (width + cols), transcendentals=rows * cols),
    )(ids, h, low_gate, low_up, w_gate, w_up, b_gate, b_up)


def attention_kernel(ids_ref, h_ref, low_ref, w_q_ref, w_k_ref, w_v_ref, b_q_ref, b_k_ref, b_v_ref, a_o_ref, cos_ref, sin_ref, out_ref, low_o_ref, sum_ref):
    rows = h_ref.shape[0]
    seq_len, head_dim = cos_ref.shape
    head = pl.program_id(0)

    @pl.when(head == 0)
    def _():
        sum_ref[...] = jnp.zeros_like(sum_ref)

    h = h_ref[...]
    both = jnp.dot(h, jnp.concatenate([w_q_ref[0], w_k_ref[0]], axis=1), preferred_element_type=jnp.float32)
    base_v = jnp.dot(h, w_v_ref[0], preferred_element_type=jnp.float32)
    cos, sin = cos_ref[...], sin_ref[...]
    causal = lax.broadcasted_iota(jnp.int32, (seq_len, seq_len), 0) >= lax.broadcasted_iota(jnp.int32, (seq_len, seq_len), 1)

    def rope(z):
        return (z * cos + pltpu.roll(z, head_dim // 2, 1) * sin).astype(jnp.bfloat16)

    for seq in range(rows // seq_len):
        part = slice(seq * seq_len, (seq + 1) * seq_len)
        at = pl.ds(seq * seq_len, seq_len)
        adapter = ids_ref[seq]

        def delta(index, b_ref):
            return jnp.dot(low_ref[index, at, :], b_ref[adapter, 0], preferred_element_type=jnp.float32)

        q = rope(both[part, :head_dim] + delta(0, b_q_ref))
        k = rope(both[part, head_dim:] + delta(1, b_k_ref))
        v = (base_v[part] + delta(2, b_v_ref)).astype(jnp.bfloat16)
        scores = lax.dot_general(q, k, NT, preferred_element_type=jnp.float32) * head_dim ** -0.5
        scores = jnp.where(causal, scores, -1e30)
        prob = jnp.exp(scores - jnp.max(scores, axis=-1, keepdims=True))
        prob = (prob / jnp.sum(prob, axis=-1, keepdims=True)).astype(jnp.bfloat16)
        mixed = jnp.dot(prob, v, preferred_element_type=jnp.float32).astype(jnp.bfloat16)
        out_ref[at, :] = mixed
        sum_ref[at, :] += jnp.dot(mixed, a_o_ref[adapter, 0], preferred_element_type=jnp.float32)

    @pl.when(head == pl.num_programs(0) - 1)
    def _():
        low_o_ref[...] = sum_ref[...].astype(low_o_ref.dtype)


def attention(ids, h, low, w_q, w_k, w_v, b_q, b_k, b_v, a_o, cos, sin):
    rows, width = h.shape
    heads, _, head_dim = w_q.shape
    adapters, _, rank, _ = b_q.shape
    w_spec = pl.BlockSpec((1, width, head_dim), lambda n, ids: (n, 0, 0))
    b_spec = pl.BlockSpec((adapters, 1, rank, head_dim), lambda n, ids: (0, n, 0, 0))
    a_spec = pl.BlockSpec((adapters, 1, head_dim, rank), lambda n, ids: (0, n, 0, 0))
    flops = 6 * rows * (width + 2 * rank) * heads * head_dim
    return pl.pallas_call(
        attention_kernel,
        out_shape=(jax.ShapeDtypeStruct((rows, heads * head_dim), jnp.bfloat16), jax.ShapeDtypeStruct((rows, rank), jnp.bfloat16)),
        grid_spec=pltpu.PrefetchScalarGridSpec(
            num_scalar_prefetch=1,
            grid=(heads,),
            in_specs=[whole((rows, width)), whole(low.shape), w_spec, w_spec, w_spec, b_spec, b_spec, b_spec, a_spec, whole(cos.shape), whole(sin.shape)],
            out_specs=(pl.BlockSpec((rows, head_dim), lambda n, ids: (0, n)), pl.BlockSpec((rows, rank), lambda n, ids: (0, 0))),
            scratch_shapes=[pltpu.VMEM((rows, rank), jnp.float32)],
        ),
        compiler_params=pltpu.CompilerParams(dimension_semantics=('arbitrary',), vmem_limit_bytes=VMEM_LIMIT),
        cost_estimate=pl.CostEstimate(flops=flops, bytes_accessed=6 * width * heads * head_dim + 2 * rows * width, transcendentals=rows * 128 * heads),
    )(ids, h, low, w_q, w_k, w_v, b_q, b_k, b_v, a_o, cos, sin)


def solution(mesh):
    tp_size = mesh.shape['tensor']
    head_split = P(None, 'tensor', None)
    last_split = P(None, None, 'tensor')
    b_head_split = P(None, None, 'tensor', None)
    in_specs = (P('data', None, None), P('data'), P(None), P(None),
                head_split, head_split, head_split, P('tensor', None, None),
                P(None, 'tensor'), P(None, 'tensor'), P('tensor', None),
                last_split, b_head_split, last_split, b_head_split, last_split, b_head_split,
                P(None, 'tensor', None, None), last_split,
                last_split, last_split, last_split, last_split,
                P(None, 'tensor', None), last_split)

    def local_layer(x_in, adapter_ids, gain_attn, gain_mlp, w_q, w_k, w_v, w_o, w_gate, w_up, w_down, a_q, b_q, a_k, b_k, a_v, b_v, a_o, b_o, a_gate, b_gate, a_up, b_up, a_down, b_down):
        batch, seq_len, width = x_in.shape
        adapters, rank = b_q.shape[:2]
        rank_part = rank // tp_size
        scale = ALPHA / rank
        per_chunk = batch // CHUNKS
        my_index = lax.axis_index('tensor')
        shard_width = width // tp_size
        flat_b = lambda b: b.reshape((adapters * rank,) + b.shape[2:])

        def rows_a(a):
            return a.transpose(0, 2, 1).reshape(adapters * rank_part, width)

        head_first = lambda w: w.transpose(1, 0, 2)
        b_heads = lambda b: b.transpose(0, 2, 1, 3)
        swapped = lambda b: b.transpose(0, 2, 1)
        cos_tab, sin_tab = rope_tables(seq_len, w_q.shape[2])

        def expand(low, hot):
            low = low * jnp.asarray(scale, jnp.bfloat16)
            wide = jnp.where(hot[:, None, :, None], low[:, :, None, :], jnp.zeros((), jnp.bfloat16))
            return wide.reshape(per_chunk, seq_len, adapters * rank)

        own = per_chunk // tp_size

        def after(ids, *values):
            for value in values:
                head = value[(0,) * value.ndim].astype(jnp.float32)
                ids = ids + (head > jnp.inf).astype(jnp.int32)
            return ids

        def low_own(act, stacks, hot):
            lows = []
            for a_stack in stacks:
                low = jnp.einsum('bsd,nd->bsn', act, rows_a(a_stack), preferred_element_type=jnp.float32)
                low = low.reshape(per_chunk, seq_len, adapters, rank_part)
                lows.append(jnp.sum(jnp.where(hot[:, None, :, None], low, 0.0), axis=2).astype(jnp.bfloat16))
            return jnp.concatenate(lows, axis=-1)

        def low_all(low, count):
            full = lax.all_gather(low, 'tensor', axis=0)
            full = full.reshape(tp_size, per_chunk, seq_len, count, rank_part)
            return full.transpose(3, 1, 2, 0, 4).reshape(count, per_chunk, seq_len, rank)

        def swap(value, bit):
            return lax.ppermute(value, 'tensor', [(i, i ^ bit) for i in range(tp_size)])

        def pick(value, index, axis):
            return lax.squeeze(lax.dynamic_slice_in_dim(value, index, 1, axis=axis), (axis,))

        def add(left, right):
            return (left.astype(jnp.float32) + right.astype(jnp.float32)).astype(jnp.bfloat16)

        core, col, row = my_index % 2, (my_index // 2) % 2, my_index // 4

        def low_sum(low_part):
            for bit in (1, 2, 4):
                low_part = add(low_part, swap(low_part, bit))
            return low_part

        def scatter_sum(key, part):
            half = seq_len // 2
            part = part.reshape(4, 2, seq_len, width)
            got = swap(pick(part, 1 - core, 1), 1)
            part = add(pick(part, core, 1), got).reshape(2, 2, seq_len, width)
            first[key] = part
            by_col, by_row = part[:, :, :half], part[:, :, half:]
            got_col = swap(pick(by_col, 1 - col, 1), 2)
            got_row = swap(pick(by_row, 1 - row, 0), 4)
            by_col = add(pick(by_col, col, 1), got_col)
            by_row = add(pick(by_row, row, 0), got_row)
            second[key] = by_row
            got_col = swap(pick(by_col, 1 - row, 0), 4)
            got_row = swap(pick(by_row, 1 - col, 0), 2)
            by_col = add(pick(by_col, row, 0), got_col)
            by_row = add(pick(by_row, col, 0), got_row)
            return jnp.concatenate([by_col, by_row], axis=0)[None]

        def chunk_of(c):
            ids = lax.slice_in_dim(adapter_ids, c * per_chunk, (c + 1) * per_chunk)
            return ids, ids[:, None] == jnp.arange(adapters)[None, :]

        def flat(value):
            return value.reshape(per_chunk * seq_len, value.shape[-1])

        def attn_low(c):
            x_c = lax.slice_in_dim(x_in, c * per_chunk, (c + 1) * per_chunk)
            h_attn = rms_gain(x_c, gain_attn)
            low = low_all(low_own(h_attn, (a_q, a_k, a_v), chunk_of(c)[1]), 3) * jnp.asarray(scale, jnp.bfloat16)
            return flat(h_attn), low.reshape(3, per_chunk * seq_len, rank)

        def attn_mix(c, *values):
            h_attn, low = pre[c]
            mixed, low_part = attention(after(chunk_of(c)[0], *values), h_attn, low, *map(head_first, (w_q, w_k, w_v)), *map(b_heads, (b_q, b_k, b_v)), a_o, cos_tab, sin_tab)
            act['a', c] = mixed
            base['a', c] = jnp.einsum('tk,kd->td', mixed, w_o.reshape(-1, width), preferred_element_type=jnp.float32).astype(jnp.bfloat16)
            low_sums['a', c] = low_sum(low_part)

        def whole_part(key, c, b_stack):
            low = low_sums[key, c].reshape(per_chunk, seq_len, rank)
            delta = jnp.einsum('tk,kd->td', flat(expand(low, chunk_of(c)[1])), flat_b(b_stack), preferred_element_type=jnp.float32)
            start = my_index * shard_width
            mine = lax.dynamic_slice_in_dim(base[key, c], start, shard_width, axis=1)
            mine = (mine.astype(jnp.float32) + delta).astype(jnp.bfloat16)
            part = lax.dynamic_update_slice_in_dim(base[key, c], mine, start, axis=1)
            return part.reshape(per_chunk, seq_len, width)

        def attn_out(c):
            part_o[c] = whole_part('a', c, b_o)
            z_o = scatter_sum(('a', c), part_o[c]) if c else lax.psum_scatter(part_o[c], 'tensor', scatter_dimension=0, tiled=True)
            x_own = lax.dynamic_slice_in_dim(x_in, c * per_chunk + my_index * own, own, axis=0)
            mid[c] = (x_own.astype(jnp.float32) + z_o.astype(jnp.float32)).astype(jnp.bfloat16)
            h_own[c] = rms_gain(mid[c], gain_mlp)
            h_mlp[c] = lax.all_gather(h_own[c], 'tensor', axis=0, tiled=True)

        def mlp_mix(c, *values):
            ids = chunk_of(c)[0]
            late = after(ids, act['m', c - 1]) if c else ids
            low = low_all(low_own(h_mlp[c], (a_gate, a_up), late[:, None] == jnp.arange(adapters)[None, :]), 2)
            low_gu[c] = low.reshape(2, per_chunk * seq_len, rank) * jnp.asarray(scale, jnp.bfloat16)
            act['m', c] = gate_up(after(ids, *values), flat(h_mlp[c]), low_gu[c][0], low_gu[c][1], w_gate.T, w_up.T, swapped(b_gate), swapped(b_up))
            a_sel = jnp.take(a_down, ids, axis=0, mode='clip')
            low_part = jnp.einsum('bsf,bfr->bsr', act['m', c].reshape(per_chunk, seq_len, -1), a_sel, preferred_element_type=jnp.float32).astype(jnp.bfloat16)
            low_sums['m', c] = low_sum(flat(low_part))
            base['m', c] = jnp.einsum('tk,kd->td', act['m', c], w_down, preferred_element_type=jnp.float32).astype(jnp.bfloat16)

        def mlp_out(c):
            part_d[c] = whole_part('m', c, b_down)
            z_down = scatter_sum(('m', c), part_d[c]) if c in (1, 2) else lax.psum_scatter(part_d[c], 'tensor', scatter_dimension=0, tiled=True)
            y_own[c] = (mid[c].astype(jnp.float32) + z_down.astype(jnp.float32)).astype(jnp.bfloat16)
            return lax.all_gather(y_own[c], 'tensor', axis=0, tiled=True)

        pre, act, base, low_sums, part_o, part_d, mid, h_mlp, low_gu, y_own, y_all, h_own, first, second = ({} for _ in range(14))
        for c in range(CHUNKS):
            pre[c] = attn_low(c)
        attn_mix(0)
        attn_mix(1, act['a', 0])
        attn_out(0)
        attn_mix(2, act['a', 1], part_o[0])
        attn_out(1)
        attn_mix(3, act['a', 2], h_own[0], first['a', 1])
        attn_out(2)
        attn_out(3)
        mlp_mix(0, act['a', 3], part_o[3], h_own[1], first['a', 2])
        y_all[0] = mlp_out(0)
        mlp_mix(1, act['m', 0], part_d[0], h_mlp[2], first['a', 3])
        y_all[1] = mlp_out(1)
        mlp_mix(2, act['m', 1], part_d[1], h_own[3], y_own[0])
        y_all[2] = mlp_out(2)
        mlp_mix(3, act['m', 2], part_d[2], y_all[0], y_own[1])
        y_all[3] = mlp_out(3)
        out = jnp.zeros_like(x_in)
        for c in range(CHUNKS):
            out = lax.dynamic_update_slice_in_dim(out, y_all[c], c * per_chunk, axis=0)
        return out

    return jax.shard_map(local_layer, mesh=mesh, in_specs=in_specs, out_specs=P('data', None, None), check_vma=False)
```

```python
import jax
import jax.numpy as jnp
from jax import lax
from jax.experimental import pallas as pl
from jax.experimental.pallas import tpu as pltpu
from jax.sharding import PartitionSpec as P

ALPHA = 16.0
ROPE_BASE = 10000.0
EPSILON = 1e-5
CHUNKS = 4


def rms_gain(act_in, gain_vec):
    act_f32 = act_in.astype(jnp.float32)
    inv_rms = lax.rsqrt(jnp.mean(act_f32 * act_f32, axis=-1, keepdims=True) + EPSILON)
    return (act_f32 * inv_rms * gain_vec).astype(jnp.bfloat16)


def rope_tables(seq_len, head_dim):
    half_dim = head_dim // 2
    inv_freq = ROPE_BASE ** (-2.0 * jnp.arange(half_dim, dtype=jnp.float32) / head_dim)
    angle_tab = jnp.arange(seq_len, dtype=jnp.float32)[:, None] * inv_freq[None, :]
    cos_tab, sin_tab = jnp.cos(angle_tab), jnp.sin(angle_tab)
    return jnp.concatenate([cos_tab, cos_tab], axis=-1), jnp.concatenate([-sin_tab, sin_tab], axis=-1)


COLS = 256
NT = (((1,), (1,)), ((), ()))
VMEM_LIMIT = 46 * 1024 * 1024


def whole(shape):
    return pl.BlockSpec(shape, lambda n, ids: (0,) * len(shape), pipeline_mode=pl.Buffered(1))


def gate_up_kernel(ids_ref, h_ref, low_gate_ref, low_up_ref, w_gate_ref, w_up_ref, b_gate_ref, b_up_ref, out_ref):
    rows = h_ref.shape[0]
    seq_len = rows // ids_ref.shape[0]

    def proj(w_ref, b_ref, low_ref):
        deltas = []
        for seq in range(rows // seq_len):
            low = low_ref[pl.ds(seq * seq_len, seq_len), :]
            deltas.append(lax.dot_general(low, b_ref[ids_ref[seq]], NT, preferred_element_type=jnp.float32))
        base = lax.dot_general(h_ref[...], w_ref[...], NT, preferred_element_type=jnp.float32)
        return base + jnp.concatenate(deltas, axis=0)

    z_gate = proj(w_gate_ref, b_gate_ref, low_gate_ref)
    z_up = proj(w_up_ref, b_up_ref, low_up_ref)
    out_ref[...] = (z_gate * jax.nn.sigmoid(z_gate) * z_up).astype(out_ref.dtype)


def gate_up(ids, h, low_gate, low_up, w_gate, w_up, b_gate, b_up):
    rows, width = h.shape
    cols = w_gate.shape[0]
    adapters, _, rank = b_gate.shape
    w_spec = pl.BlockSpec((COLS, width), lambda n, ids: (n, 0))
    b_spec = pl.BlockSpec((adapters, COLS, rank), lambda n, ids: (0, n, 0))
    flops = 4 * rows * (width + rank) * cols
    return pl.pallas_call(
        gate_up_kernel,
        out_shape=jax.ShapeDtypeStruct((rows, cols), jnp.bfloat16),
        grid_spec=pltpu.PrefetchScalarGridSpec(
            num_scalar_prefetch=1,
            grid=(pl.cdiv(cols, COLS),),
            in_specs=[whole((rows, width)), whole((rows, rank)), whole((rows, rank)), w_spec, w_spec, b_spec, b_spec],
            out_specs=pl.BlockSpec((rows, COLS), lambda n, ids: (0, n)),
        ),
        compiler_params=pltpu.CompilerParams(dimension_semantics=('arbitrary',), vmem_limit_bytes=VMEM_LIMIT),
        cost_estimate=pl.CostEstimate(flops=flops, bytes_accessed=4 * width * cols + 2 * rows * (width + cols), transcendentals=rows * cols),
    )(ids, h, low_gate, low_up, w_gate, w_up, b_gate, b_up)


def attention_kernel(ids_ref, h_ref, low_ref, w_q_ref, w_k_ref, w_v_ref, b_q_ref, b_k_ref, b_v_ref, a_o_ref, cos_ref, sin_ref, out_ref, low_o_ref, sum_ref):
    rows = h_ref.shape[0]
    seq_len, head_dim = cos_ref.shape
    head = pl.program_id(0)

    @pl.when(head == 0)
    def _():
        sum_ref[...] = jnp.zeros_like(sum_ref)

    h = h_ref[...]
    both = jnp.dot(h, jnp.concatenate([w_q_ref[0], w_k_ref[0]], axis=1), preferred_element_type=jnp.float32)
    base_v = jnp.dot(h, w_v_ref[0], preferred_element_type=jnp.float32)
    cos, sin = cos_ref[...], sin_ref[...]
    causal = lax.broadcasted_iota(jnp.int32, (seq_len, seq_len), 0) >= lax.broadcasted_iota(jnp.int32, (seq_len, seq_len), 1)

    def rope(z):
        return (z * cos + pltpu.roll(z, head_dim // 2, 1) * sin).astype(jnp.bfloat16)

    for seq in range(rows // seq_len):
        part = slice(seq * seq_len, (seq + 1) * seq_len)
        at = pl.ds(seq * seq_len, seq_len)
        adapter = ids_ref[seq]

        def delta(index, b_ref):
            return jnp.dot(low_ref[index, at, :], b_ref[adapter, 0], preferred_element_type=jnp.float32)

        q = rope(both[part, :head_dim] + delta(0, b_q_ref))
        k = rope(both[part, head_dim:] + delta(1, b_k_ref))
        v = (base_v[part] + delta(2, b_v_ref)).astype(jnp.bfloat16)
        scores = lax.dot_general(q, k, NT, preferred_element_type=jnp.float32) * head_dim ** -0.5
        scores = jnp.where(causal, scores, -1e30)
        prob = jnp.exp(scores - jnp.max(scores, axis=-1, keepdims=True))
        prob = (prob / jnp.sum(prob, axis=-1, keepdims=True)).astype(jnp.bfloat16)
        mixed = jnp.dot(prob, v, preferred_element_type=jnp.float32).astype(jnp.bfloat16)
        out_ref[at, :] = mixed
        sum_ref[at, :] += jnp.dot(mixed, a_o_ref[adapter, 0], preferred_element_type=jnp.float32)

    @pl.when(head == pl.num_programs(0) - 1)
    def _():
        low_o_ref[...] = sum_ref[...].astype(low_o_ref.dtype)


def attention(ids, h, low, w_q, w_k, w_v, b_q, b_k, b_v, a_o, cos, sin):
    rows, width = h.shape
    heads, _, head_dim = w_q.shape
    adapters, _, rank, _ = b_q.shape
    w_spec = pl.BlockSpec((1, width, head_dim), lambda n, ids: (n, 0, 0))
    b_spec = pl.BlockSpec((adapters, 1, rank, head_dim), lambda n, ids: (0, n, 0, 0))
    a_spec = pl.BlockSpec((adapters, 1, head_dim, rank), lambda n, ids: (0, n, 0, 0))
    flops = 6 * rows * (width + 2 * rank) * heads * head_dim
    return pl.pallas_call(
        attention_kernel,
        out_shape=(jax.ShapeDtypeStruct((rows, heads * head_dim), jnp.bfloat16), jax.ShapeDtypeStruct((rows, rank), jnp.bfloat16)),
        grid_spec=pltpu.PrefetchScalarGridSpec(
            num_scalar_prefetch=1,
            grid=(heads,),
            in_specs=[whole((rows, width)), whole(low.shape), w_spec, w_spec, w_spec, b_spec, b_spec, b_spec, a_spec, whole(cos.shape), whole(sin.shape)],
            out_specs=(pl.BlockSpec((rows, head_dim), lambda n, ids: (0, n)), pl.BlockSpec((rows, rank), lambda n, ids: (0, 0))),
            scratch_shapes=[pltpu.VMEM((rows, rank), jnp.float32)],
        ),
        compiler_params=pltpu.CompilerParams(dimension_semantics=('arbitrary',), vmem_limit_bytes=VMEM_LIMIT),
        cost_estimate=pl.CostEstimate(flops=flops, bytes_accessed=6 * width * heads * head_dim + 2 * rows * width, transcendentals=rows * 128 * heads),
    )(ids, h, low, w_q, w_k, w_v, b_q, b_k, b_v, a_o, cos, sin)


def solution(mesh):
    tp_size = mesh.shape['tensor']
    head_split = P(None, 'tensor', None)
    last_split = P(None, None, 'tensor')
    b_head_split = P(None, None, 'tensor', None)
    in_specs = (P('data', None, None), P('data'), P(None), P(None),
                head_split, head_split, head_split, P('tensor', None, None),
                P(None, 'tensor'), P(None, 'tensor'), P('tensor', None),
                last_split, b_head_split, last_split, b_head_split, last_split, b_head_split,
                P(None, 'tensor', None, None), last_split,
                last_split, last_split, last_split, last_split,
                P(None, 'tensor', None), last_split)

    def local_layer(x_in, adapter_ids, gain_attn, gain_mlp, w_q, w_k, w_v, w_o, w_gate, w_up, w_down, a_q, b_q, a_k, b_k, a_v, b_v, a_o, b_o, a_gate, b_gate, a_up, b_up, a_down, b_down):
        batch, seq_len, width = x_in.shape
        adapters, rank = b_q.shape[:2]
        rank_part = rank // tp_size
        scale = ALPHA / rank
        per_chunk = batch // CHUNKS
        my_index = lax.axis_index('tensor')
        shard_width = width // tp_size
        flat_b = lambda b: b.reshape((adapters * rank,) + b.shape[2:])

        def rows_a(a):
            return a.transpose(0, 2, 1).reshape(adapters * rank_part, width)

        head_first = lambda w: w.transpose(1, 0, 2)
        b_heads = lambda b: b.transpose(0, 2, 1, 3)
        swapped = lambda b: b.transpose(0, 2, 1)
        cos_tab, sin_tab = rope_tables(seq_len, w_q.shape[2])

        def expand(low, hot):
            low = low * jnp.asarray(scale, jnp.bfloat16)
            wide = jnp.where(hot[:, None, :, None], low[:, :, None, :], jnp.zeros((), jnp.bfloat16))
            return wide.reshape(per_chunk, seq_len, adapters * rank)

        own = per_chunk // tp_size

        def after(ids, *values):
            for value in values:
                head = value[(0,) * value.ndim].astype(jnp.float32)
                ids = ids + (head > jnp.inf).astype(jnp.int32)
            return ids

        def low_own(act, stacks, hot):
            lows = []
            for a_stack in stacks:
                low = jnp.einsum('bsd,nd->bsn', act, rows_a(a_stack), preferred_element_type=jnp.float32)
                low = low.reshape(per_chunk, seq_len, adapters, rank_part)
                lows.append(jnp.sum(jnp.where(hot[:, None, :, None], low, 0.0), axis=2).astype(jnp.bfloat16))
            return jnp.concatenate(lows, axis=-1)

        def low_all(low, count):
            full = lax.all_gather(low, 'tensor', axis=0)
            full = full.reshape(tp_size, per_chunk, seq_len, count, rank_part)
            return full.transpose(3, 1, 2, 0, 4).reshape(count, per_chunk, seq_len, rank)

        def swap(value, bit):
            return lax.ppermute(value, 'tensor', [(i, i ^ bit) for i in range(tp_size)])

        def add(left, right):
            return (left.astype(jnp.float32) + right.astype(jnp.float32)).astype(jnp.bfloat16)

        def low_sum(low_part):
            for bit in (1, 2, 4):
                low_part = add(low_part, swap(low_part, bit))
            return low_part

        def chunk_of(c):
            ids = lax.slice_in_dim(adapter_ids, c * per_chunk, (c + 1) * per_chunk)
            return ids, ids[:, None] == jnp.arange(adapters)[None, :]

        def flat(value):
            return value.reshape(per_chunk * seq_len, value.shape[-1])

        def attn_low(c, *values):
            x_c = lax.dynamic_slice_in_dim(x_in, after(jnp.int32(c * per_chunk), *values), per_chunk, axis=0)
            h_attn = rms_gain(x_c, gain_attn)
            seen[c] = low_own(h_attn, (a_q, a_k, a_v), chunk_of(c)[1])
            low = low_all(seen[c], 3) * jnp.asarray(scale, jnp.bfloat16)
            return flat(h_attn), low.reshape(3, per_chunk * seq_len, rank)

        def attn_mix(c, *values):
            h_attn, low = pre[c]
            mixed, low_part = attention(after(chunk_of(c)[0], *values), h_attn, low, *map(head_first, (w_q, w_k, w_v)), *map(b_heads, (b_q, b_k, b_v)), a_o, cos_tab, sin_tab)
            act['a', c] = mixed
            base['a', c] = jnp.einsum('tk,kd->td', mixed, w_o.reshape(-1, width), preferred_element_type=jnp.float32).astype(jnp.bfloat16)
            low_sums['a', c] = low_sum(low_part)

        def whole_part(key, c, b_stack):
            low = low_sums[key, c].reshape(per_chunk, seq_len, rank)
            delta = jnp.einsum('tk,kd->td', flat(expand(low, chunk_of(c)[1])), flat_b(b_stack), preferred_element_type=jnp.float32)
            start = my_index * shard_width
            mine = lax.dynamic_slice_in_dim(base[key, c], start, shard_width, axis=1)
            mine = (mine.astype(jnp.float32) + delta).astype(jnp.bfloat16)
            part = lax.dynamic_update_slice_in_dim(base[key, c], mine, start, axis=1)
            return part.reshape(per_chunk, seq_len, width)

        def attn_out(c):
            part_o[c] = whole_part('a', c, b_o)
            z_o = lax.psum_scatter(part_o[c], 'tensor', scatter_dimension=0, tiled=True)
            start = after(c * per_chunk + my_index * own, *([h_own[c - 1]] if c else []))
            x_own = lax.dynamic_slice_in_dim(x_in, start, own, axis=0)
            mid[c] = (x_own.astype(jnp.float32) + z_o.astype(jnp.float32)).astype(jnp.bfloat16)
            h_own[c] = rms_gain(mid[c], gain_mlp)
            h_mlp[c] = lax.all_gather(h_own[c], 'tensor', axis=0, tiled=True)

        def mlp_mix(c, *values):
            ids = chunk_of(c)[0]
            low = low_all(low_own(h_mlp[c], (a_gate, a_up), chunk_of(c)[1]), 2)
            low_gu[c] = low.reshape(2, per_chunk * seq_len, rank) * jnp.asarray(scale, jnp.bfloat16)
            act['m', c] = gate_up(after(ids, *values), flat(h_mlp[c]), low_gu[c][0], low_gu[c][1], w_gate.T, w_up.T, swapped(b_gate), swapped(b_up))
            a_sel = jnp.take(a_down, ids, axis=0, mode='clip')
            low_part = jnp.einsum('bsf,bfr->bsr', act['m', c].reshape(per_chunk, seq_len, -1), a_sel, preferred_element_type=jnp.float32).astype(jnp.bfloat16)
            low_sums['m', c] = low_sum(flat(low_part))
            base['m', c] = jnp.einsum('tk,kd->td', act['m', c], w_down, preferred_element_type=jnp.float32).astype(jnp.bfloat16)

        def mlp_out(c):
            part_d[c] = whole_part('m', c, b_down)
            z_down = lax.psum_scatter(part_d[c], 'tensor', scatter_dimension=0, tiled=True)
            y_own[c] = (mid[c].astype(jnp.float32) + z_down.astype(jnp.float32)).astype(jnp.bfloat16)
            return lax.all_gather(y_own[c], 'tensor', axis=0, tiled=True)

        pre, act, base, low_sums, part_o, part_d, mid, h_mlp, low_gu, y_own, y_all, h_own, seen = ({} for _ in range(13))
        pre[0] = attn_low(0)
        pre[1] = attn_low(1, seen[0])
        attn_mix(0)
        pre[2] = attn_low(2, act['a', 0])
        attn_mix(1, act['a', 0])
        pre[3] = attn_low(3, act['a', 1])
        attn_out(0)
        attn_mix(2, act['a', 1], h_own[0])
        attn_out(1)
        attn_mix(3, act['a', 2], h_own[1], h_mlp[0])
        attn_out(2)
        attn_out(3)
        mlp_mix(0, act['a', 3], part_o[3], h_own[2], h_mlp[1])
        y_all[0] = mlp_out(0)
        mlp_mix(1, act['m', 0], part_d[0], h_own[3], h_mlp[2])
        y_all[1] = mlp_out(1)
        mlp_mix(2, act['m', 1], part_d[1], y_own[0], h_mlp[3])
        y_all[2] = mlp_out(2)
        mlp_mix(3, act['m', 2], part_d[2], y_own[1], y_all[0])
        y_all[3] = mlp_out(3)
        out = jnp.zeros_like(x_in)
        for c in range(CHUNKS):
            out = lax.dynamic_update_slice_in_dim(out, y_all[c], c * per_chunk, axis=0)
        return out

    return jax.shard_map(local_layer, mesh=mesh, in_specs=in_specs, out_specs=P('data', None, None), check_vma=False)
```
